32 devices in a mesh: rows: 16 (over z, y, x), cols: 2 (over core).
Axes of the slice: x: 2, y: 2, z: 4, core: 2. Of those that a mesh axis runs over, the one named last changes fastest.
Arguments:
- embeddings: bfloat16 [49152, 1536], P('rows'), may hold values from -43 to 43, as said below
- start_basis: float32 [1536, 256], P(None, 'cols'), may hold values from -6 to 6
Outputs:
- projected: bfloat16 [49152, 256], P('rows', 'cols')
- basis: float32 [1536, 256], P(None, 'cols')
The draws below stay inside these ranges and needn't reach their ends.
Inputs may be any that keep to these rules, and one draw needn't show every extreme that they name: `embeddings`: rows are noisy vectors around offsets that differ between aligned blocks of rows, with per-column spreads that differ by a factor of up to four.
All inputs are finite; a program needn't handle non-finite values.
Results may differ from the reference program's by a relative error of at most 0.025.
Values may be sent and summed in bfloat16 or wider, within the bound.
A program may use at most 64 MiB of HBM per device.

```python
import jax
import jax.numpy as jnp
from jax import lax

D = 1536
K = 256
ROW_DEV = 3072
ITERS = 3
ROWS = 49152


def draw_embeddings(key, part):
    key_offset, key_scale, key_noise = jax.random.split(key, 3)
    key_blocks = jax.random.fold_in(key, 7919)
    offset = jnp.clip(jax.random.normal(key_offset, (D,), jnp.float32), -3.0, 3.0)
    col_scale = jnp.exp(jax.random.uniform(key_scale, (D,), jnp.float32, -0.69, 0.69))
    block_shift = jnp.clip(0.8 * jax.random.normal(key_blocks, (ROWS // ROW_DEV, D), jnp.float32), -3.0, 3.0)
    row_shift = jnp.repeat(block_shift, ROW_DEV, axis=0, total_repeat_length=ROWS)
    noise = jnp.clip(jax.random.normal(key_noise, (ROWS, D), jnp.float32), -5.0, 5.0)
    values = noise * col_scale[None, :] + offset[None, :] + row_shift
    return values.astype(jnp.bfloat16)


def block_scale(rng, extent, pieces, smallest, high):
    def one(dim, blocks):
        steps = jax.random.uniform(jax.random.fold_in(jax.random.fold_in(rng, 6), dim), (blocks,), jnp.float32, smallest / len(pieces), high / len(pieces))
        return jnp.repeat(jnp.exp(steps), extent[dim] // blocks).reshape((-1,) + (1,) * (len(extent) - dim - 1))

    gain = one(*pieces[0])
    for cut in pieces[1:]:
        gain = gain * one(*cut)
    return gain


def normal_values(own_key, shape, width, limit, cuts=(), held_as=jnp.bfloat16):
    values = width * jax.random.normal(own_key, shape, jnp.float32)
    if cuts:
        values = values * block_scale(own_key, shape, cuts, -0.22, 0.18)
    return jnp.clip(values, -limit, limit).astype(held_as)


def setup_inputs(seed: int = 0) -> dict:
    streams_of = jax.random.split(jax.random.key(seed), 3)
    return {
        "embeddings": draw_embeddings(jax.random.fold_in(streams_of[2], 71), 0),
        "start_basis": normal_values(streams_of[1], (D, K), 1.0, 6.0, ((1, 2),), jnp.float32),
    }


def reference(embeddings, start_basis):
    rows_count = embeddings.shape[0]
    col_mean = lax.optimization_barrier(jnp.sum(embeddings, axis=0, dtype=jnp.float32)) / rows_count
    basis = start_basis
    for sweep_index in range(ITERS):
        basis_bf = basis.astype(jnp.bfloat16)
        raw_proj = jnp.dot(embeddings.astype(jnp.float32), basis_bf.astype(jnp.float32), preferred_element_type=jnp.float32)
        offset = jnp.dot(col_mean, basis_bf.astype(jnp.float32), precision=lax.Precision.HIGHEST)
        shifted = (raw_proj - offset[None, :]).astype(jnp.bfloat16)
        col_sums = lax.optimization_barrier(jnp.sum(shifted, axis=0, dtype=jnp.float32))
        products = lax.dot_general(embeddings.astype(jnp.float32), shifted.astype(jnp.float32), (((0,), (0,)), ((), ())), preferred_element_type=jnp.float32)
        products = products - col_mean[:, None] * col_sums[None, :]
        gram_matrix = jnp.dot(products.T, products, precision=lax.Precision.HIGHEST)
        lower = jnp.linalg.cholesky(gram_matrix)
        basis = lax.linalg.triangular_solve(lower, products, left_side=False, lower=True, transpose_a=True)
    centered = embeddings.astype(jnp.float32) - col_mean[None, :]
    unit = (centered * lax.rsqrt(lax.optimization_barrier(jnp.sum(centered * centered, axis=1, keepdims=True)) + 1.0)).astype(jnp.bfloat16)
    coords = jnp.dot(unit.astype(jnp.float32), basis.astype(jnp.bfloat16).astype(jnp.float32), preferred_element_type=jnp.float32)
    scaled = coords * lax.rsqrt(lax.optimization_barrier(jnp.mean(coords * coords, axis=1, keepdims=True)) + 0.0001)
    return (scaled.astype(jnp.bfloat16), basis)
```

```python
import functools

import jax
import jax.numpy as jnp
from jax import lax
from jax.experimental import pallas as pl
from jax.experimental.pallas import tpu as pltpu
from jax.sharding import PartitionSpec as P

ITERS = 3
PARTS = 3
HI = lax.Precision.HIGHEST
F32 = jnp.float32
BF16 = jnp.bfloat16


def dot(a, b, ca, cb, precision=None):
    return lax.dot_general(a, b, (((ca,), (cb,)), ((), ())), precision=precision, preferred_element_type=F32)


def scatter_kernel(n, e_ref, w_ref, s_ref, acc, sums):
    step = pl.program_id(0)
    core = lax.axis_index("cols")
    t = acc.shape[1]

    @pl.when(step == 0)
    def _():
        acc[...] = jnp.zeros_like(acc)
        sums[...] = jnp.zeros_like(sums)

    e = e_ref[...]
    sums[...] += dot(jnp.ones((8, e.shape[0]), BF16), e, 1, 0)

    def block(slot, i, j):
        acc[slot] += dot(e[:, i * t:(i + 1) * t], e[:, j * t:(j + 1) * t], 0, 0)

    def finish(slot, i, j):
        si = sums[:, i * t:(i + 1) * t] * (1.0 / (8 * n))
        sj = sums[:, j * t:(j + 1) * t]
        w_ref[slot] = (acc[slot] - dot(si, sj, 0, 0, HI)).astype(w_ref.dtype)

    last = step == pl.num_programs(0) - 1
    for c, pairs in enumerate((((0, 0), (0, 1), (0, 2)), ((1, 1), (1, 2), (2, 2)))):
        @pl.when(core == c)
        def _(pairs=pairs):
            for slot, (i, j) in enumerate(pairs):
                block(slot, i, j)

            @pl.when(last)
            def _():
                for slot, (i, j) in enumerate(pairs):
                    finish(slot, i, j)

    @pl.when(last)
    def _():
        s_ref[...] = sums[...]


def scatter(e, rows=512):
    n, d = e.shape
    t = d // PARTS
    return pl.pallas_call(
        functools.partial(scatter_kernel, n),
        grid=(n // rows,),
        in_specs=[pl.BlockSpec((rows, d), lambda i: (i, 0))],
        out_specs=[pl.BlockSpec((PARTS, t, t), lambda i: (0, 0, 0)), pl.BlockSpec((8, d), lambda i: (0, 0))],
        out_shape=[jax.ShapeDtypeStruct((PARTS, t, t), BF16), jax.ShapeDtypeStruct((8, d), F32)],
        scratch_shapes=[pltpu.VMEM((PARTS, t, t), F32), pltpu.VMEM((8, d), F32)],
    )(e)


def inverse_factor(a_ref, k, b):
    sub = lax.broadcasted_iota(jnp.int32, (8, 2 * b), 0)
    eye = (lax.broadcasted_iota(jnp.int32, (b, b), 0) == lax.broadcasted_iota(jnp.int32, (b, b), 1)).astype(F32)
    for blk in range(k // b):
        lo, hi = blk * b, (blk + 1) * b
        aug = jnp.concatenate([a_ref[lo:hi, lo:hi], eye], axis=1)
        tiles = [aug[8 * t:8 * t + 8] for t in range(b // 8)]
        for j in range(b):
            tj, r = j // 8, j % 8
            cols = {t: jnp.broadcast_to(tiles[t][:, j:j + 1], (8, 2 * b)) for t in range(tj, b // 8)}
            row = tiles[tj][r:r + 1] * (1.0 / cols[tj][r:r + 1])
            for t in range(tj, b // 8):
                f = cols[t]
                if t == tj:
                    if r == 7:
                        continue
                    f = jnp.where(sub > r, f, 0.0)
                tiles[t] = tiles[t] - f * row
        aug = jnp.concatenate(tiles, axis=0)
        diag = jnp.sum(aug[:, :b] * eye, axis=1, keepdims=True)
        scale = lax.rsqrt(diag)
        scale = scale * (1.5 - 0.5 * diag * scale * scale)
        strip = dot(aug[:, b:] * scale, a_ref[lo:hi, :], 1, 0, HI)
        a_ref[lo:hi, :] = strip
        if hi < k:
            a_ref[hi:, :] -= dot(strip[:, hi:k], strip, 0, 0, HI)


def iterate_kernel(n, total, w_ref, s_ref, b_ref, out_ref, w, basis, mean, a):
    d, k = out_ref.shape
    t = d // PARTS
    for c, pairs in enumerate((((0, 0), (0, 1), (0, 2)), ((1, 1), (1, 2), (2, 2)))):
        for slot, (i, j) in enumerate(pairs):
            v = w_ref[c, slot]
            w[i * t:(i + 1) * t, j * t:(j + 1) * t] = v
            if i != j:
                w[j * t:(j + 1) * t, i * t:(i + 1) * t] = v.T
    s = s_ref[...]
    mean[...] = s * (1.0 / n) - jnp.sum(s, axis=0, keepdims=True) * (1.0 / total)
    basis[...] = b_ref[...]

    @pl.loop(0, ITERS)
    def _(_):
        bf = basis[...]
        m = mean[...]
        inner = dot(m, bf.astype(F32), 1, 0, HI) * float(n)
        products = dot(w[...], bf, 1, 0) + dot(m, inner, 0, 0, HI)
        a[:, :k] = dot(products, products, 0, 0, HI)
        a[:, k:] = (
            lax.broadcasted_iota(jnp.int32, (k, k), 0) == lax.broadcasted_iota(jnp.int32, (k, k), 1)
        ).astype(F32)
        inverse_factor(a, k, 64)
        new = dot(products, a[:, k:], 1, 1, HI)
        out_ref[...] = new
        basis[...] = new.astype(BF16)


def iterate(n, total, w, s, b):
    d, k = b.shape
    vm = pl.BlockSpec(memory_space=pltpu.VMEM)
    return pl.pallas_call(
        functools.partial(iterate_kernel, n, total),
        in_specs=[vm] * 3,
        out_specs=vm,
        out_shape=jax.ShapeDtypeStruct((d, k), F32),
        scratch_shapes=[
            pltpu.VMEM((d, d), BF16),
            pltpu.VMEM((d, k), BF16),
            pltpu.VMEM(s.shape, F32),
            pltpu.VMEM((k, 2 * k), F32),
        ],
    )(w, s, b)


def project_kernel(total, e_ref, s_ref, b_ref, o_ref, basis_ref, mean, bf):
    core = lax.axis_index("cols")
    h = o_ref.shape[1]

    @pl.when(pl.program_id(0) == 0)
    def _():
        mean[...] = jnp.sum(s_ref[...], axis=0, keepdims=True) * (1.0 / total)
        full = b_ref[...]
        bf[...] = full.astype(BF16)
        basis_ref[...] = jnp.where(core == 0, full[:, :h], full[:, h:])

    centered = e_ref[...].astype(F32) - mean[...]
    unit = (centered * lax.rsqrt(jnp.sum(centered * centered, axis=1, keepdims=True) + 1.0)).astype(BF16)
    coords = dot(unit, bf[...], 1, 0)
    k = coords.shape[1]
    scale = lax.rsqrt(jnp.sum(coords * coords, axis=1, keepdims=True) * (1.0 / k) + 0.0001)
    o_ref[...] = (jnp.where(core == 0, coords[:, :h], coords[:, h:]) * scale).astype(o_ref.dtype)


def project(total, e, s, b, h, rows=512):
    n, d = e.shape
    k = b.shape[1]
    return pl.pallas_call(
        functools.partial(project_kernel, total),
        grid=(n // rows,),
        in_specs=[
            pl.BlockSpec((rows, d), lambda i: (i, 0)),
            pl.BlockSpec(s.shape, lambda i: (0, 0)),
            pl.BlockSpec((d, k), lambda i: (0, 0)),
        ],
        out_specs=[pl.BlockSpec((rows, h), lambda i: (i, 0)), pl.BlockSpec((d, h), lambda i: (0, 0))],
        out_shape=[jax.ShapeDtypeStruct((n, h), BF16), jax.ShapeDtypeStruct((d, h), F32)],
        scratch_shapes=[pltpu.VMEM((1, d), F32), pltpu.VMEM((d, k), BF16)],
    )(e, s, b)


def shards(embeddings, start_basis):
    n, d = embeddings.shape
    total = n * lax.axis_size("rows")
    w, s = scatter(embeddings)
    w = lax.psum(w, "rows")
    w = lax.all_gather(w, "cols", axis=0)
    s = lax.all_gather(s[0], "rows", axis=0)
    b = lax.all_gather(start_basis.astype(BF16), "cols", axis=1, tiled=True)
    basis = iterate(n, total, w, s, b)
    return project(total, embeddings, s, basis, start_basis.shape[1])


def solution(mesh):
    in_specs = (P("rows", None), P(None, "cols"))
    out_specs = (P("rows", "cols"), P(None, "cols"))
    return jax.shard_map(shards, mesh=mesh, in_specs=in_specs, out_specs=out_specs, check_vma=False)
```

```python
import functools

import jax
import jax.numpy as jnp
from jax import lax
from jax.experimental import pallas as pl
from jax.experimental.pallas import tpu as pltpu
from jax.sharding import PartitionSpec as P

ITERS = 3
PARTS = 3
LANES = 128
MESH = pl.DeviceIdType.MESH
HI = lax.Precision.HIGHEST
F32 = jnp.float32
BF16 = jnp.bfloat16


def dot(a, b, ca, cb, precision=None):
    return lax.dot_general(a, b, (((ca,), (cb,)), ((), ())), precision=precision, preferred_element_type=F32)


def scatter_kernel(n, e_ref, w_ref, s_ref, acc, sums):
    step = pl.program_id(0)
    core = lax.axis_index("cols")
    t = acc.shape[1]

    @pl.when(step == 0)
    def _():
        acc[...] = jnp.zeros_like(acc)
        sums[...] = jnp.zeros_like(sums)

    e = e_ref[...]
    sums[...] += dot(jnp.ones((8, e.shape[0]), BF16), e, 1, 0)

    def block(slot, i, j):
        acc[slot] += dot(e[:, i * t:(i + 1) * t], e[:, j * t:(j + 1) * t], 0, 0)

    def finish(slot, i, j):
        si = sums[:, i * t:(i + 1) * t] * (1.0 / (8 * n))
        sj = sums[:, j * t:(j + 1) * t]
        v = (acc[slot] - dot(si, sj, 0, 0, HI)).astype(w_ref.dtype)
        for c in range(t // LANES):
            w_ref[slot, c] = v[:, c * LANES:(c + 1) * LANES]

    last = step == pl.num_programs(0) - 1
    for c, pairs in enumerate((((0, 0), (0, 1), (0, 2)), ((1, 1), (1, 2), (2, 2)))):
        @pl.when(core == c)
        def _(pairs=pairs):
            for slot, (i, j) in enumerate(pairs):
                block(slot, i, j)

            @pl.when(last)
            def _():
                for slot, (i, j) in enumerate(pairs):
                    finish(slot, i, j)

    @pl.when(last)
    def _():
        s_ref[...] = sums[0:1, :]


def scatter(e, rows=512):
    n, d = e.shape
    t = d // PARTS
    return pl.pallas_call(
        functools.partial(scatter_kernel, n),
        grid=(n // rows,),
        in_specs=[pl.BlockSpec((rows, d), lambda i: (i, 0))],
        out_specs=[
            pl.BlockSpec((PARTS, t // LANES, t, LANES), lambda i: (0, 0, 0, 0)),
            pl.BlockSpec((1, d), lambda i: (0, 0)),
        ],
        out_shape=[
            jax.ShapeDtypeStruct((PARTS, t // LANES, t, LANES), BF16),
            jax.ShapeDtypeStruct((1, d), F32),
        ],
        scratch_shapes=[pltpu.VMEM((PARTS, t, t), F32), pltpu.VMEM((8, d), F32)],
    )(e)


def inverse_factor(a_ref, k, b):
    sub = lax.broadcasted_iota(jnp.int32, (8, 2 * b), 0)
    eye = (lax.broadcasted_iota(jnp.int32, (b, b), 0) == lax.broadcasted_iota(jnp.int32, (b, b), 1)).astype(F32)
    for blk in range(k // b):
        lo, hi = blk * b, (blk + 1) * b
        aug = jnp.concatenate([a_ref[lo:hi, lo:hi], eye], axis=1)
        tiles = [aug[8 * t:8 * t + 8] for t in range(b // 8)]
        for j in range(b):
            tj, r = j // 8, j % 8
            cols = {t: jnp.broadcast_to(tiles[t][:, j:j + 1], (8, 2 * b)) for t in range(tj, b // 8)}
            row = tiles[tj][r:r + 1] * (1.0 / cols[tj][r:r + 1])
            for t in range(tj, b // 8):
                f = cols[t]
                if t == tj:
                    if r == 7:
                        continue
                    f = jnp.where(sub > r, f, 0.0)
                tiles[t] = tiles[t] - f * row
        aug = jnp.concatenate(tiles, axis=0)
        diag = jnp.sum(aug[:, :b] * eye, axis=1, keepdims=True)
        scale = lax.rsqrt(diag)
        scale = scale * (1.5 - 0.5 * diag * scale * scale)
        strip = dot(aug[:, b:] * scale, a_ref[lo:hi, :], 1, 0, HI)
        a_ref[lo:hi, :] = strip
        if hi < k:
            a_ref[hi:, :] -= dot(strip[:, hi:k], strip, 0, 0, HI)


def iterate_kernel(n, total, w_ref, s_ref, b_ref, out_ref, w, basis, mean, a):
    d, k = out_ref.shape
    t = d // PARTS
    for c, pairs in enumerate((((0, 0), (0, 1), (0, 2)), ((1, 1), (1, 2), (2, 2)))):
        for slot, (i, j) in enumerate(pairs):
            v = jnp.concatenate([w_ref[c, slot, l] for l in range(t // LANES)], axis=1)
            w[i * t:(i + 1) * t, j * t:(j + 1) * t] = v
            if i != j:
                w[j * t:(j + 1) * t, i * t:(i + 1) * t] = v.T
    s = s_ref[:, 0, :]
    mean[...] = s * (1.0 / n) - jnp.sum(s, axis=0, keepdims=True) * (1.0 / total)
    basis[...] = jnp.concatenate([b_ref[0], b_ref[1]], axis=1)

    @pl.loop(0, ITERS)
    def _(_):
        bf = basis[...]
        m = mean[...]
        inner = dot(m, bf.astype(F32), 1, 0, HI) * float(n)
        products = dot(w[...], bf, 1, 0) + dot(m, inner, 0, 0, HI)
        a[:, :k] = dot(products, products, 0, 0, HI)
        a[:, k:] = (
            lax.broadcasted_iota(jnp.int32, (k, k), 0) == lax.broadcasted_iota(jnp.int32, (k, k), 1)
        ).astype(F32)
        inverse_factor(a, k, 64)
        new = dot(products, a[:, k:], 1, 1, HI)
        out_ref[...] = new
        basis[...] = new.astype(BF16)


def iterate(n, total, w, s, b):
    d, k = b.shape[1], 2 * b.shape[2]
    vm = pl.BlockSpec(memory_space=pltpu.VMEM)
    return pl.pallas_call(
        functools.partial(iterate_kernel, n, total),
        in_specs=[vm] * 3,
        out_specs=vm,
        out_shape=jax.ShapeDtypeStruct((d, k), F32),
        scratch_shapes=[
            pltpu.VMEM((d, d), BF16),
            pltpu.VMEM((d, k), BF16),
            pltpu.VMEM((s.shape[0], d), F32),
            pltpu.VMEM((k, 2 * k), F32),
        ],
    )(w, s, b)


def project_kernel(total, e_ref, s_ref, b_ref, o_ref, basis_ref, mean, bf):
    core = lax.axis_index("cols")
    h = o_ref.shape[1]

    @pl.when(pl.program_id(0) == 0)
    def _():
        mean[...] = jnp.sum(s_ref[:, 0, :], axis=0, keepdims=True) * (1.0 / total)
        full = b_ref[...]
        bf[...] = full.astype(BF16)
        basis_ref[...] = jnp.where(core == 0, full[:, :h], full[:, h:])

    centered = e_ref[...].astype(F32) - mean[...]
    unit = (centered * lax.rsqrt(jnp.sum(centered * centered, axis=1, keepdims=True) + 1.0)).astype(BF16)
    coords = dot(unit, bf[...], 1, 0)
    k = coords.shape[1]
    scale = lax.rsqrt(jnp.sum(coords * coords, axis=1, keepdims=True) * (1.0 / k) + 0.0001)
    o_ref[...] = (jnp.where(core == 0, coords[:, :h], coords[:, h:]) * scale).astype(o_ref.dtype)


def project(total, e, s, b, h, rows=512):
    n, d = e.shape
    k = b.shape[1]
    return pl.pallas_call(
        functools.partial(project_kernel, total),
        grid=(n // rows,),
        in_specs=[
            pl.BlockSpec((rows, d), lambda i: (i, 0)),
            pl.BlockSpec(s.shape, lambda i: (0, 0, 0)),
            pl.BlockSpec((d, k), lambda i: (0, 0)),
        ],
        out_specs=[pl.BlockSpec((rows, h), lambda i: (i, 0)), pl.BlockSpec((d, h), lambda i: (0, 0))],
        out_shape=[jax.ShapeDtypeStruct((n, h), BF16), jax.ShapeDtypeStruct((d, h), F32)],
        scratch_shapes=[pltpu.VMEM((1, d), F32), pltpu.VMEM((d, k), BF16)],
    )(e, s, b)


def factors(r):
    z = 4 if r % 4 == 0 else 1
    x = 1
    while x * x < r // z:
        x *= 2
    return z, r // z // x, x


def reduce_kernel(r, w_ref, s_ref, b_ref, wout, sout, bout, *scratch):
    nz, ny, nx = factors(r)
    plans = (("x", "y", "z"), ("y", "x", "z"))
    size = {"x": nx, "y": ny, "z": nz}
    stride = {"x": 1, "y": nx, "z": nx * ny}
    scratch = list(scratch)
    stage = [[scratch.pop(0) for _ in plan] for plan in plans]
    held = [[scratch.pop(0) for _ in plan[:-1]] for plan in plans]
    w_send, w_recv, s_send, s_recv, c_send, c_recv = scratch

    me = lax.axis_index("rows")
    core = lax.axis_index("cols")
    at = {a: lax.rem(me // stride[a], size[a]) for a in size}
    partner = {"cols": 1 - core}

    def peer(a, k):
        p = lax.rem(at[a] + k, size[a])
        return p, {"rows": me + (p - at[a]) * stride[a]}

    barrier = pltpu.get_barrier_semaphore()
    count = 1
    pl.semaphore_signal(barrier, inc=1, device_id=partner, device_id_type=MESH)
    for a in size:
        for k in range(1, size[a]):
            pl.semaphore_signal(barrier, inc=1, device_id=peer(a, k)[1], device_id_type=MESH)
            count += 1
    pl.semaphore_wait(barrier, count)

    def remote(src, dst, send, recv, device):
        copy = pltpu.make_async_remote_copy(
            src_ref=src, dst_ref=dst, send_sem=send, recv_sem=recv, device_id=device, device_id_type=MESH
        )
        copy.start()
        return copy

    def rows_of(off, m):
        return pl.ds(pl.multiple_of(off, 16), m)

    length = w_ref.shape[0]
    off = [q * (length // 2) for q in range(2)]
    span = [length // 2] * 2

    def start_reduce(q, ph):
        a = plans[q][ph]
        g = size[a]
        m = span[q] // g
        copies = []
        for k in range(1, g):
            p, dev = peer(a, k)
            src = w_ref.at[rows_of(off[q] + p * m, m)] if ph == 0 else held[q][ph - 1].at[rows_of(p * m, m)]
            copies.append(
                remote(src, stage[q][ph].at[k - 1], w_send.at[q, ph, k - 1], w_recv.at[q, ph, k - 1], dev)
            )
        return copies

    def finish_reduce(q, ph, copies):
        a = plans[q][ph]
        g = size[a]
        m = span[q] // g
        for c in copies:
            c.wait()
        mine = rows_of(off[q] + at[a] * m, m) if ph == 0 else rows_of(at[a] * m, m)
        total = (w_ref[mine] if ph == 0 else held[q][ph - 1][mine]).astype(F32)
        for k in range(g - 1):
            total = total + stage[q][ph][k].astype(F32)
        off[q] = off[q] + at[a] * m
        span[q] = m
        if ph < len(plans[q]) - 1:
            held[q][ph][...] = total.astype(BF16)
        else:
            wout[core, rows_of(off[q], m)] = total.astype(BF16)

    def start_sums(ph):
        a = "xyz"[ph]
        width = stride[a]
        first = me // width * width
        block = pl.ds(first, width)
        return [
            remote(sout.at[block], sout.at[block], s_send.at[ph, k - 1], s_recv.at[ph, k - 1], peer(a, k)[1])
            for k in range(1, size[a])
        ]

    sout[me] = s_ref[...]
    bout[core] = b_ref[...]
    pending = [start_reduce(q, 0) for q in range(2)]
    sums = start_sums(0)
    basis_copy = remote(b_ref, bout.at[core], c_send.at[2], c_recv.at[2], partner)
    for ph in range(3):
        for c in sums:
            c.wait()
        if ph < 2:
            sums = start_sums(ph + 1)
        for q in range(2):
            finish_reduce(q, ph, pending[q])
            if ph < 2:
                pending[q] = start_reduce(q, ph + 1)

    def start_gather(q, ph):
        a = plans[q][ph]
        block = wout.at[core, rows_of(off[q], span[q])]
        return [
            remote(block, block, w_send.at[q, 3 + ph, k - 1], w_recv.at[q, 3 + ph, k - 1], peer(a, k)[1])
            for k in range(1, size[a])
        ]

    pending = [start_gather(q, 2) for q in range(2)]
    across = []
    for ph in (2, 1, 0):
        for q in range(2):
            a = plans[q][ph]
            for c in pending[q]:
                c.wait()
            off[q] = off[q] - at[a] * span[q]
            span[q] = span[q] * size[a]
            if ph > 0:
                pending[q] = start_gather(q, ph - 1)
            if ph == 1:
                early = rows_of(off[q], span[q])
                block = wout.at[core, early]
                across.append(remote(block, block, c_send.at[q], c_recv.at[q], partner))
    for q in range(2):
        a = plans[q][0]
        part = span[q] // size[a]
        for k in range(1, size[a]):
            p = peer(a, k)[0]
            block = wout.at[core, rows_of(off[q] + p * part, part)]
            across.append(remote(block, block, c_send.at[2 + q * 3 + k], c_recv.at[2 + q * 3 + k], partner))
    for c in across:
        c.wait()
    basis_copy.wait()


def reduce(r, w, s, b):
    length = w.shape[0]
    nz, ny, nx = factors(r)
    stages, helds = [], []
    for sizes in ((nx, ny, nz), (ny, nx, nz)):
        m = length // 2
        for ph, g in enumerate(sizes):
            m //= g
            stages.append(pltpu.VMEM((max(g - 1, 1), m, LANES), BF16))
            if ph < 2:
                helds.append(pltpu.VMEM((m, LANES), BF16))
    widest = max(nx, ny, nz) - 1
    vm = pl.BlockSpec(memory_space=pltpu.VMEM)
    dma = pltpu.SemaphoreType.DMA
    return pl.pallas_call(
        functools.partial(reduce_kernel, r),
        in_specs=[vm] * 3,
        out_specs=[vm] * 3,
        out_shape=[
            jax.ShapeDtypeStruct((2,) + w.shape, BF16),
            jax.ShapeDtypeStruct((r,) + s.shape, F32),
            jax.ShapeDtypeStruct((2,) + b.shape, BF16),
        ],
        scratch_shapes=stages + helds + [dma((2, 6, widest)), dma((2, 6, widest)), dma((3, widest)), dma((3, widest)), dma((9,)), dma((9,))],
        compiler_params=pltpu.CompilerParams(collective_id=0, has_side_effects=True),
    )(w, s, b)


def shards(embeddings, start_basis):
    n, d = embeddings.shape
    total = n * lax.axis_size("rows")
    w, s = scatter(embeddings)
    shape = w.shape
    w, s, b = reduce(lax.axis_size("rows"), w.reshape(-1, LANES), s, start_basis.astype(BF16))
    w = w.reshape((2,) + shape)
    basis = iterate(n, total, w, s, b)
    return project(total, embeddings, s, basis, start_basis.shape[1])


def solution(mesh):
    in_specs = (P("rows", None), P(None, "cols"))
    out_specs = (P("rows", "cols"), P(None, "cols"))
    return jax.shard_map(shards, mesh=mesh, in_specs=in_specs, out_specs=out_specs, check_vma=False)
```

```python
import functools

import jax
import jax.numpy as jnp
from jax import lax
from jax.experimental import pallas as pl
from jax.experimental.pallas import tpu as pltpu
from jax.sharding import PartitionSpec as P

ITERS = 3
PARTS = 3
LANES = 128
MESH = pl.DeviceIdType.MESH
HI = lax.Precision.HIGHEST
F32 = jnp.float32
BF16 = jnp.bfloat16


def dot(a, b, ca, cb, precision=None):
    return lax.dot_general(a, b, (((ca,), (cb,)), ((), ())), precision=precision, preferred_element_type=F32)


def scatter_kernel(n, e_ref, w_ref, s_ref, acc, sums):
    step = pl.program_id(0)
    core = lax.axis_index("cols")
    t = acc.shape[1]

    @pl.when(step == 0)
    def _():
        acc[...] = jnp.zeros_like(acc)
        sums[...] = jnp.zeros_like(sums)

    e = e_ref[...]
    sums[...] += dot(jnp.ones((8, e.shape[0]), BF16), e, 1, 0)

    def block(slot, i, j):
        acc[slot] += dot(e[:, i * t:(i + 1) * t], e[:, j * t:(j + 1) * t], 0, 0)

    def finish(slot, i, j):
        si = sums[:, i * t:(i + 1) * t] * (1.0 / (8 * n))
        sj = sums[:, j * t:(j + 1) * t]
        v = (acc[slot] - dot(si, sj, 0, 0, HI)).astype(w_ref.dtype)
        for c in range(t // LANES):
            w_ref[slot, c] = v[:, c * LANES:(c + 1) * LANES]

    last = step == pl.num_programs(0) - 1
    for c, pairs in enumerate((((0, 0), (0, 1), (0, 2)), ((1, 1), (1, 2), (2, 2)))):
        @pl.when(core == c)
        def _(pairs=pairs):
            for slot, (i, j) in enumerate(pairs):
                block(slot, i, j)

            @pl.when(last)
            def _():
                for slot, (i, j) in enumerate(pairs):
                    finish(slot, i, j)

    @pl.when(last)
    def _():
        s_ref[...] = sums[0:1, :]


def scatter(e, rows=512):
    n, d = e.shape
    t = d // PARTS
    return pl.pallas_call(
        functools.partial(scatter_kernel, n),
        grid=(n // rows,),
        in_specs=[pl.BlockSpec((rows, d), lambda i: (i, 0))],
        out_specs=[
            pl.BlockSpec((PARTS, t // LANES, t, LANES), lambda i: (0, 0, 0, 0)),
            pl.BlockSpec((1, d), lambda i: (0, 0)),
        ],
        out_shape=[
            jax.ShapeDtypeStruct((PARTS, t // LANES, t, LANES), BF16),
            jax.ShapeDtypeStruct((1, d), F32),
        ],
        scratch_shapes=[pltpu.VMEM((PARTS, t, t), F32), pltpu.VMEM((8, d), F32)],
    )(e)


def split(v):
    hi = v.astype(BF16)
    return hi, (v - hi.astype(F32)).astype(BF16)


def pivot_inverse(a):
    m = len(a)
    a = [list(row) for row in a]
    t = [[None] * m for _ in range(m)]
    inv = []
    for j in range(m):
        r = 1.0 / a[j][j]
        inv.append(r)
        for i in range(j + 1, m):
            f = a[i][j] * r
            for c in range(j + 1, i + 1):
                a[i][c] = a[i][c] - f * a[c][j]
            for c in range(j):
                t[i][c] = t[i][c] - f * t[j][c]
            t[i][j] = -f
    return t, inv


def inverse_factor(a_ref, k, b):
    w = 2 * b
    sub = lax.broadcasted_iota(jnp.int32, (8, w), 0)
    eye = (lax.broadcasted_iota(jnp.int32, (b, b), 0) == lax.broadcasted_iota(jnp.int32, (b, b), 1)).astype(F32)
    for blk in range(k // b):
        lo, hi = blk * b, (blk + 1) * b
        aug = jnp.concatenate([a_ref[lo:hi, lo:hi], eye], axis=1)
        tiles = [aug[8 * t:8 * t + 8] for t in range(b // 8)]
        for p in range(b // 8):
            cols = {
                t: [jnp.broadcast_to(tiles[t][:, 8 * p + c:8 * p + c + 1], (8, w)) for c in range(8)]
                for t in range(p, b // 8)
            }
            block = [[jnp.broadcast_to(cols[p][j][i:i + 1], (8, w)) for j in range(i + 1)] for i in range(8)]
            t8, inv = pivot_inverse(block)
            rows = [jnp.broadcast_to(tiles[p][c:c + 1], (8, w)) for c in range(8)]
            low = []
            for i in range(8):
                v = rows[i]
                for c in range(i):
                    v = v + t8[i][c] * rows[c]
                low.append(v)
            scaled = [low[i] * inv[i] for i in range(8)]
            if p + 1 < b // 8:
                solved = []
                for c in range(8):
                    v = scaled[c]
                    for i in range(c + 1, 8):
                        v = v + t8[i][c] * scaled[i]
                    solved.append(v)
                for t in range(p + 1, b // 8):
                    u = [cols[t][c] * solved[c] for c in range(8)]
                    tiles[t] = tiles[t] - (((u[0] + u[1]) + (u[2] + u[3])) + ((u[4] + u[5]) + (u[6] + u[7])))
            v, d = low[0], inv[0]
            for i in range(1, 8):
                v = jnp.where(sub == i, low[i], v)
                d = jnp.where(sub == i, inv[i], d)
            root = lax.rsqrt(d)
            root = root * (1.5 - 0.5 * d * root * root)
            tiles[p] = v * (d * root)
        strip = dot(jnp.concatenate(tiles, axis=0)[:, b:], a_ref[lo:hi, :], 1, 0, HI)
        a_ref[lo:hi, :] = strip
        if hi < k:
            a_ref[hi:, :] -= dot(strip[:, hi:k], strip, 0, 0, HI)


def iterate_kernel(n, total, w_ref, s_ref, b_ref, out_ref, w, basis, mean, mean_t, a):
    d, k = out_ref.shape
    t = d // PARTS
    for c, pairs in enumerate((((0, 0), (0, 1), (0, 2)), ((1, 1), (1, 2), (2, 2)))):
        for slot, (i, j) in enumerate(pairs):
            v = jnp.concatenate([w_ref[c, slot, l] for l in range(t // LANES)], axis=1)
            w[i * t:(i + 1) * t, j * t:(j + 1) * t] = v
            if i != j:
                w[j * t:(j + 1) * t, i * t:(i + 1) * t] = v.T
    s = s_ref[:, 0, :]
    r = s.shape[0]
    m = s * (1.0 / n) - jnp.sum(s, axis=0, keepdims=True) * (1.0 / total)
    mh, ml = split(m)
    mean[:r] = mh
    mean[r:] = ml
    mean_t[...] = jnp.concatenate([mh.astype(F32), ml.astype(F32), mh.astype(F32)], axis=0).T.astype(BF16)
    basis[...] = jnp.concatenate([b_ref[0], b_ref[1]], axis=1)

    @pl.loop(0, ITERS)
    def _(_):
        bf = basis[...]
        inner = dot(mean[...], bf, 1, 0)
        ih, il = split((inner[:r] + inner[r:]) * float(n))
        ph, plo = split(dot(w[...], bf, 1, 0) + dot(mean_t[...], jnp.concatenate([ih, ih, il], axis=0), 1, 0))
        cross = dot(plo, ph, 0, 0)
        a[:, :k] = dot(ph, ph, 0, 0) + (dot(plo, plo, 0, 0) + (cross + cross.T))
        a[:, k:] = (
            lax.broadcasted_iota(jnp.int32, (k, k), 0) == lax.broadcasted_iota(jnp.int32, (k, k), 1)
        ).astype(F32)
        inverse_factor(a, k, 64)
        lh, ll = split(a[:, k:])
        new = dot(ph, lh, 1, 1) + (dot(ph, ll, 1, 1) + dot(plo, lh, 1, 1))
        out_ref[...] = new
        basis[...] = new.astype(BF16)


def iterate(n, total, w, s, b):
    d, k = b.shape[1], 2 * b.shape[2]
    vm = pl.BlockSpec(memory_space=pltpu.VMEM)
    return pl.pallas_call(
        functools.partial(iterate_kernel, n, total),
        in_specs=[vm] * 3,
        out_specs=vm,
        out_shape=jax.ShapeDtypeStruct((d, k), F32),
        scratch_shapes=[
            pltpu.VMEM((d, d), BF16),
            pltpu.VMEM((d, k), BF16),
            pltpu.VMEM((2 * s.shape[0], d), BF16),
            pltpu.VMEM((d, 3 * s.shape[0]), BF16),
            pltpu.VMEM((k, 2 * k), F32),
        ],
    )(w, s, b)


def project_kernel(total, e_ref, s_ref, b_ref, o_ref, basis_ref, mean, bf):
    core = lax.axis_index("cols")
    h = o_ref.shape[1]

    @pl.when(pl.program_id(0) == 0)
    def _():
        mean[...] = jnp.sum(s_ref[:, 0, :], axis=0, keepdims=True) * (1.0 / total)
        full = b_ref[...]
        bf[...] = full.astype(BF16)
        basis_ref[...] = jnp.where(core == 0, full[:, :h], full[:, h:])

    centered = e_ref[...].astype(F32) - mean[...]
    unit = (centered * lax.rsqrt(jnp.sum(centered * centered, axis=1, keepdims=True) + 1.0)).astype(BF16)
    coords = dot(unit, bf[...], 1, 0)
    k = coords.shape[1]
    scale = lax.rsqrt(jnp.sum(coords * coords, axis=1, keepdims=True) * (1.0 / k) + 0.0001)
    o_ref[...] = (jnp.where(core == 0, coords[:, :h], coords[:, h:]) * scale).astype(o_ref.dtype)


def project(total, e, s, b, h, rows=512):
    n, d = e.shape
    k = b.shape[1]
    return pl.pallas_call(
        functools.partial(project_kernel, total),
        grid=(n // rows,),
        in_specs=[
            pl.BlockSpec((rows, d), lambda i: (i, 0)),
            pl.BlockSpec(s.shape, lambda i: (0, 0, 0)),
            pl.BlockSpec((d, k), lambda i: (0, 0)),
        ],
        out_specs=[pl.BlockSpec((rows, h), lambda i: (i, 0)), pl.BlockSpec((d, h), lambda i: (0, 0))],
        out_shape=[jax.ShapeDtypeStruct((n, h), BF16), jax.ShapeDtypeStruct((d, h), F32)],
        scratch_shapes=[pltpu.VMEM((1, d), F32), pltpu.VMEM((d, k), BF16)],
    )(e, s, b)


def factors(r):
    z = 4 if r % 4 == 0 else 1
    x = 1
    while x * x < r // z:
        x *= 2
    return z, r // z // x, x


def reduce_kernel(r, w_ref, s_ref, b_ref, wout, sout, bout, *scratch):
    nz, ny, nx = factors(r)
    plans = (("x", "y", "z"), ("y", "x", "z"))
    size = {"x": nx, "y": ny, "z": nz}
    stride = {"x": 1, "y": nx, "z": nx * ny}
    scratch = list(scratch)
    stage = [[scratch.pop(0) for _ in plan] for plan in plans]
    held = [[scratch.pop(0) for _ in plan[:-1]] for plan in plans]
    w_send, w_recv, s_send, s_recv, c_send, c_recv = scratch

    me = lax.axis_index("rows")
    core = lax.axis_index("cols")
    at = {a: lax.rem(me // stride[a], size[a]) for a in size}
    partner = {"cols": 1 - core}

    def peer(a, k):
        p = lax.rem(at[a] + k, size[a])
        return p, {"rows": me + (p - at[a]) * stride[a]}

    barrier = pltpu.get_barrier_semaphore()
    count = 1
    pl.semaphore_signal(barrier, inc=1, device_id=partner, device_id_type=MESH)
    for a in size:
        for k in range(1, size[a]):
            pl.semaphore_signal(barrier, inc=1, device_id=peer(a, k)[1], device_id_type=MESH)
            count += 1
    pl.semaphore_wait(barrier, count)

    def remote(src, dst, send, recv, device):
        copy = pltpu.make_async_remote_copy(
            src_ref=src, dst_ref=dst, send_sem=send, recv_sem=recv, device_id=device, device_id_type=MESH
        )
        copy.start()
        return copy

    def rows_of(off, m):
        return pl.ds(pl.multiple_of(off, 16), m)

    length = w_ref.shape[0]
    off = [q * (length // 2) for q in range(2)]
    span = [length // 2] * 2

    def start_reduce(q, ph):
        a = plans[q][ph]
        g = size[a]
        m = span[q] // g
        copies = []
        for k in range(1, g):
            p, dev = peer(a, k)
            src = w_ref.at[rows_of(off[q] + p * m, m)] if ph == 0 else held[q][ph - 1].at[rows_of(p * m, m)]
            copies.append(
                remote(src, stage[q][ph].at[k - 1], w_send.at[q, ph, k - 1], w_recv.at[q, ph, k - 1], dev)
            )
        return copies

    def finish_reduce(q, ph, copies):
        a = plans[q][ph]
        g = size[a]
        m = span[q] // g
        for c in copies:
            c.wait()
        mine = rows_of(off[q] + at[a] * m, m) if ph == 0 else rows_of(at[a] * m, m)
        total = (w_ref[mine] if ph == 0 else held[q][ph - 1][mine]).astype(F32)
        for k in range(g - 1):
            total = total + stage[q][ph][k].astype(F32)
        off[q] = off[q] + at[a] * m
        span[q] = m
        if ph < len(plans[q]) - 1:
            held[q][ph][...] = total.astype(BF16)
        else:
            wout[core, rows_of(off[q], m)] = total.astype(BF16)

    def start_sums(ph):
        a = "xyz"[ph]
        width = stride[a]
        first = me // width * width
        block = pl.ds(first, width)
        return [
            remote(sout.at[block], sout.at[block], s_send.at[ph, k - 1], s_recv.at[ph, k - 1], peer(a, k)[1])
            for k in range(1, size[a])
        ]

    sout[me] = s_ref[...]
    bout[core] = b_ref[...]
    pending = [start_reduce(q, 0) for q in range(2)]
    sums = start_sums(0)
    basis_copy = remote(b_ref, bout.at[core], c_send.at[2], c_recv.at[2], partner)
    for ph in range(3):
        for c in sums:
            c.wait()
        if ph < 2:
            sums = start_sums(ph + 1)
        for q in range(2):
            finish_reduce(q, ph, pending[q])
            if ph < 2:
                pending[q] = start_reduce(q, ph + 1)

    def start_gather(q, ph):
        a = plans[q][ph]
        block = wout.at[core, rows_of(off[q], span[q])]
        return [
            remote(block, block, w_send.at[q, 3 + ph, k - 1], w_recv.at[q, 3 + ph, k - 1], peer(a, k)[1])
            for k in range(1, size[a])
        ]

    pending = [start_gather(q, 2) for q in range(2)]
    across = []
    for ph in (2, 1, 0):
        for q in range(2):
            a = plans[q][ph]
            for c in pending[q]:
                c.wait()
            off[q] = off[q] - at[a] * span[q]
            span[q] = span[q] * size[a]
            if ph > 0:
                pending[q] = start_gather(q, ph - 1)
            if ph == 1:
                early = rows_of(off[q], span[q])
                block = wout.at[core, early]
                across.append(remote(block, block, c_send.at[q], c_recv.at[q], partner))
    for q in range(2):
        a = plans[q][0]
        part = span[q] // size[a]
        for k in range(1, size[a]):
            p = peer(a, k)[0]
            block = wout.at[core, rows_of(off[q] + p * part, part)]
            across.append(remote(block, block, c_send.at[2 + q * 3 + k], c_recv.at[2 + q * 3 + k], partner))
    for c in across:
        c.wait()
    basis_copy.wait()


def reduce(r, w, s, b):
    length = w.shape[0]
    nz, ny, nx = factors(r)
    stages, helds = [], []
    for sizes in ((nx, ny, nz), (ny, nx, nz)):
        m = length // 2
        for ph, g in enumerate(sizes):
            m //= g
            stages.append(pltpu.VMEM((max(g - 1, 1), m, LANES), BF16))
            if ph < 2:
                helds.append(pltpu.VMEM((m, LANES), BF16))
    widest = max(nx, ny, nz) - 1
    vm = pl.BlockSpec(memory_space=pltpu.VMEM)
    dma = pltpu.SemaphoreType.DMA
    return pl.pallas_call(
        functools.partial(reduce_kernel, r),
        in_specs=[vm] * 3,
        out_specs=[vm] * 3,
        out_shape=[
            jax.ShapeDtypeStruct((2,) + w.shape, BF16),
            jax.ShapeDtypeStruct((r,) + s.shape, F32),
            jax.ShapeDtypeStruct((2,) + b.shape, BF16),
        ],
        scratch_shapes=stages + helds + [dma((2, 6, widest)), dma((2, 6, widest)), dma((3, widest)), dma((3, widest)), dma((9,)), dma((9,))],
        compiler_params=pltpu.CompilerParams(collective_id=0, has_side_effects=True),
    )(w, s, b)


def shards(embeddings, start_basis):
    n, d = embeddings.shape
    total = n * lax.axis_size("rows")
    w, s = scatter(embeddings)
    shape = w.shape
    w, s, b = reduce(lax.axis_size("rows"), w.reshape(-1, LANES), s, start_basis.astype(BF16))
    w = w.reshape((2,) + shape)
    basis = iterate(n, total, w, s, b)
    return project(total, embeddings, s, basis, start_basis.shape[1])


def solution(mesh):
    in_specs = (P("rows", None), P(None, "cols"))
    out_specs = (P("rows", "cols"), P(None, "cols"))
    return jax.shard_map(shards, mesh=mesh, in_specs=in_specs, out_specs=out_specs, check_vma=False)
```

```python
import functools

import jax
import jax.numpy as jnp
from jax import lax
from jax.experimental import pallas as pl
from jax.experimental.pallas import tpu as pltpu
from jax.sharding import PartitionSpec as P

ITERS = 3
PARTS = 3
LANES = 128
MESH = pl.DeviceIdType.MESH
STREAMS = 2 * PARTS
HI = lax.Precision.HIGHEST
F32 = jnp.float32
BF16 = jnp.bfloat16


def dot(a, b, ca, cb, precision=None):
    return lax.dot_general(a, b, (((ca,), (cb,)), ((), ())), precision=precision, preferred_element_type=F32)


def scatter_kernel(n, e_ref, w_ref, s_ref, acc, sums):
    step = pl.program_id(0)
    core = lax.axis_index("cols")
    t = acc.shape[1]

    @pl.when(step == 0)
    def _():
        acc[...] = jnp.zeros_like(acc)
        sums[...] = jnp.zeros_like(sums)

    e = e_ref[...]
    sums[...] += dot(jnp.ones((8, e.shape[0]), BF16), e, 1, 0)

    def block(slot, i, j):
        acc[slot] += dot(e[:, i * t:(i + 1) * t], e[:, j * t:(j + 1) * t], 0, 0)

    def finish(slot, i, j):
        si = sums[:, i * t:(i + 1) * t] * (1.0 / (8 * n))
        sj = sums[:, j * t:(j + 1) * t]
        v = (acc[slot] - dot(si, sj, 0, 0, HI)).astype(w_ref.dtype)
        for c in range(t // LANES):
            w_ref[slot, c] = v[:, c * LANES:(c + 1) * LANES]

    last = step == pl.num_programs(0) - 1
    for c, pairs in enumerate((((0, 0), (0, 1), (0, 2)), ((1, 1), (1, 2), (2, 2)))):
        @pl.when(core == c)
        def _(pairs=pairs):
            for slot, (i, j) in enumerate(pairs):
                block(slot, i, j)

            @pl.when(last)
            def _():
                for slot, (i, j) in enumerate(pairs):
                    finish(slot, i, j)

    @pl.when(last)
    def _():
        s_ref[...] = sums[0:1, :]


def scatter(e, rows=512):
    n, d = e.shape
    t = d // PARTS
    return pl.pallas_call(
        functools.partial(scatter_kernel, n),
        grid=(n // rows,),
        in_specs=[pl.BlockSpec((rows, d), lambda i: (i, 0))],
        out_specs=[
            pl.BlockSpec((PARTS, t // LANES, t, LANES), lambda i: (0, 0, 0, 0)),
            pl.BlockSpec((1, d), lambda i: (0, 0)),
        ],
        out_shape=[
            jax.ShapeDtypeStruct((PARTS, t // LANES, t, LANES), BF16),
            jax.ShapeDtypeStruct((1, d), F32),
        ],
        scratch_shapes=[pltpu.VMEM((PARTS, t, t), F32), pltpu.VMEM((8, d), F32)],
    )(e)


def split(v):
    hi = v.astype(BF16)
    return hi, (v - hi.astype(F32)).astype(BF16)


def pivot_inverse(a):
    m = len(a)
    a = [list(row) for row in a]
    t = [[None] * m for _ in range(m)]
    inv = []
    for j in range(m):
        r = 1.0 / a[j][j]
        inv.append(r)
        for i in range(j + 1, m):
            f = a[i][j] * r
            for c in range(j + 1, i + 1):
                a[i][c] = a[i][c] - f * a[c][j]
            for c in range(j):
                t[i][c] = t[i][c] - f * t[j][c]
            t[i][j] = -f
    return t, inv


def inverse_factor(a_ref, k, b):
    w = 2 * b
    sub = lax.broadcasted_iota(jnp.int32, (8, w), 0)
    eye = (lax.broadcasted_iota(jnp.int32, (b, b), 0) == lax.broadcasted_iota(jnp.int32, (b, b), 1)).astype(F32)
    for blk in range(k // b):
        lo, hi = blk * b, (blk + 1) * b
        aug = jnp.concatenate([a_ref[lo:hi, lo:hi], eye], axis=1)
        tiles = [aug[8 * t:8 * t + 8] for t in range(b // 8)]
        for p in range(b // 8):
            cols = {
                t: [jnp.broadcast_to(tiles[t][:, 8 * p + c:8 * p + c + 1], (8, w)) for c in range(8)]
                for t in range(p, b // 8)
            }
            block = [[jnp.broadcast_to(cols[p][j][i:i + 1], (8, w)) for j in range(i + 1)] for i in range(8)]
            t8, inv = pivot_inverse(block)
            rows = [jnp.broadcast_to(tiles[p][c:c + 1], (8, w)) for c in range(8)]
            low = []
            for i in range(8):
                v = rows[i]
                for c in range(i):
                    v = v + t8[i][c] * rows[c]
                low.append(v)
            scaled = [low[i] * inv[i] for i in range(8)]
            if p + 1 < b // 8:
                solved = []
                for c in range(8):
                    v = scaled[c]
                    for i in range(c + 1, 8):
                        v = v + t8[i][c] * scaled[i]
                    solved.append(v)
                for t in range(p + 1, b // 8):
                    u = [cols[t][c] * solved[c] for c in range(8)]
                    tiles[t] = tiles[t] - (((u[0] + u[1]) + (u[2] + u[3])) + ((u[4] + u[5]) + (u[6] + u[7])))
            v, d = low[0], inv[0]
            for i in range(1, 8):
                v = jnp.where(sub == i, low[i], v)
                d = jnp.where(sub == i, inv[i], d)
            root = lax.rsqrt(d)
            root = root * (1.5 - 0.5 * d * root * root)
            tiles[p] = v * (d * root)
        strip = dot(jnp.concatenate(tiles, axis=0)[:, b:], a_ref[lo:hi, :], 1, 0, HI)
        a_ref[lo:hi, :] = strip
        if hi < k:
            a_ref[hi:, :] -= dot(strip[:, hi:k], strip, 0, 0, HI)


def iterate_kernel(n, total, w_ref, s_ref, b_ref, out_ref, w, basis, mean, mean_t, a):
    d, k = out_ref.shape
    t = d // PARTS
    for c, pairs in enumerate((((0, 0), (0, 1), (0, 2)), ((1, 1), (1, 2), (2, 2)))):
        for slot, (i, j) in enumerate(pairs):
            v = jnp.concatenate([w_ref[c, slot, l] for l in range(t // LANES)], axis=1)
            w[i * t:(i + 1) * t, j * t:(j + 1) * t] = v
            if i != j:
                w[j * t:(j + 1) * t, i * t:(i + 1) * t] = v.T
    s = s_ref[:, 0, :]
    r = s.shape[0]
    m = s * (1.0 / n) - jnp.sum(s, axis=0, keepdims=True) * (1.0 / total)
    mh, ml = split(m)
    mean[:r] = mh
    mean[r:] = ml
    mean_t[...] = jnp.concatenate([mh.astype(F32), ml.astype(F32), mh.astype(F32)], axis=0).T.astype(BF16)
    basis[...] = jnp.concatenate([b_ref[0], b_ref[1]], axis=1)

    @pl.loop(0, ITERS)
    def _(_):
        bf = basis[...]
        inner = dot(mean[...], bf, 1, 0)
        ih, il = split((inner[:r] + inner[r:]) * float(n))
        ph, plo = split(dot(w[...], bf, 1, 0) + dot(mean_t[...], jnp.concatenate([ih, ih, il], axis=0), 1, 0))
        cross = dot(plo, ph, 0, 0)
        a[:, :k] = dot(ph, ph, 0, 0) + (dot(plo, plo, 0, 0) + (cross + cross.T))
        a[:, k:] = (
            lax.broadcasted_iota(jnp.int32, (k, k), 0) == lax.broadcasted_iota(jnp.int32, (k, k), 1)
        ).astype(F32)
        inverse_factor(a, k, 64)
        lh, ll = split(a[:, k:])
        new = dot(ph, lh, 1, 1) + (dot(ph, ll, 1, 1) + dot(plo, lh, 1, 1))
        out_ref[...] = new
        basis[...] = new.astype(BF16)


def iterate(n, total, w, s, b):
    d, k = b.shape[1], 2 * b.shape[2]
    vm = pl.BlockSpec(memory_space=pltpu.VMEM)
    return pl.pallas_call(
        functools.partial(iterate_kernel, n, total),
        in_specs=[vm] * 3,
        out_specs=vm,
        out_shape=jax.ShapeDtypeStruct((d, k), F32),
        scratch_shapes=[
            pltpu.VMEM((d, d), BF16),
            pltpu.VMEM((d, k), BF16),
            pltpu.VMEM((2 * s.shape[0], d), BF16),
            pltpu.VMEM((d, 3 * s.shape[0]), BF16),
            pltpu.VMEM((k, 2 * k), F32),
        ],
    )(w, s, b)


def project_kernel(total, e_ref, s_ref, b_ref, o_ref, basis_ref, mean, bf):
    core = lax.axis_index("cols")
    h = o_ref.shape[1]

    @pl.when(pl.program_id(0) == 0)
    def _():
        mean[...] = jnp.sum(s_ref[:, 0, :], axis=0, keepdims=True) * (1.0 / total)
        full = b_ref[...]
        bf[...] = full.astype(BF16)
        basis_ref[...] = jnp.where(core == 0, full[:, :h], full[:, h:])

    centered = e_ref[...].astype(F32) - mean[...]
    unit = (centered * lax.rsqrt(jnp.sum(centered * centered, axis=1, keepdims=True) + 1.0)).astype(BF16)
    coords = dot(unit, bf[...], 1, 0)
    k = coords.shape[1]
    scale = lax.rsqrt(jnp.sum(coords * coords, axis=1, keepdims=True) * (1.0 / k) + 0.0001)
    o_ref[...] = (jnp.where(core == 0, coords[:, :h], coords[:, h:]) * scale).astype(o_ref.dtype)


def project(total, e, s, b, h, rows=512):
    n, d = e.shape
    k = b.shape[1]
    return pl.pallas_call(
        functools.partial(project_kernel, total),
        grid=(n // rows,),
        in_specs=[
            pl.BlockSpec((rows, d), lambda i: (i, 0)),
            pl.BlockSpec(s.shape, lambda i: (0, 0, 0)),
            pl.BlockSpec((d, k), lambda i: (0, 0)),
        ],
        out_specs=[pl.BlockSpec((rows, h), lambda i: (i, 0)), pl.BlockSpec((d, h), lambda i: (0, 0))],
        out_shape=[jax.ShapeDtypeStruct((n, h), BF16), jax.ShapeDtypeStruct((d, h), F32)],
        scratch_shapes=[pltpu.VMEM((1, d), F32), pltpu.VMEM((d, k), BF16)],
    )(e, s, b)


def factors(r):
    z = 4 if r % 4 == 0 else 1
    x = 1
    while x * x < r // z:
        x *= 2
    return z, r // z // x, x


def reduce_kernel(r, w_ref, s_ref, b_ref, wout, sout, bout, *scratch):
    nz, ny, nx = factors(r)
    plans = (("x", "y", "z"), ("y", "x", "z")) * (STREAMS // 2)
    size = {"x": nx, "y": ny, "z": nz}
    stride = {"x": 1, "y": nx, "z": nx * ny}
    scratch = list(scratch)
    stage = [[scratch.pop(0) for _ in plan] for plan in plans]
    held = [[scratch.pop(0) for _ in plan[:-1]] for plan in plans]
    w_send, w_recv, s_send, s_recv, c_send, c_recv = scratch

    me = lax.axis_index("rows")
    core = lax.axis_index("cols")
    at = {a: lax.rem(me // stride[a], size[a]) for a in size}
    partner = {"cols": 1 - core}

    def peer(a, k):
        p = lax.rem(at[a] + k, size[a])
        return p, {"rows": me + (p - at[a]) * stride[a]}

    barrier = pltpu.get_barrier_semaphore()
    count = 1
    pl.semaphore_signal(barrier, inc=1, device_id=partner, device_id_type=MESH)
    for a in size:
        for k in range(1, size[a]):
            pl.semaphore_signal(barrier, inc=1, device_id=peer(a, k)[1], device_id_type=MESH)
            count += 1
    pl.semaphore_wait(barrier, count)

    def remote(src, dst, send, recv, device):
        copy = pltpu.make_async_remote_copy(
            src_ref=src, dst_ref=dst, send_sem=send, recv_sem=recv, device_id=device, device_id_type=MESH
        )
        copy.start()
        return copy

    def rows_of(off, m):
        return pl.ds(pl.multiple_of(off, 16), m)

    length = w_ref.shape[0]
    off = [q * (length // STREAMS) for q in range(STREAMS)]
    span = [length // STREAMS] * STREAMS

    def start_reduce(q, ph):
        a = plans[q][ph]
        g = size[a]
        m = span[q] // g
        copies = []
        for k in range(1, g):
            p, dev = peer(a, k)
            src = w_ref.at[rows_of(off[q] + p * m, m)] if ph == 0 else held[q][ph - 1].at[rows_of(p * m, m)]
            copies.append(
                remote(src, stage[q][ph].at[k - 1], w_send.at[q, ph, k - 1], w_recv.at[q, ph, k - 1], dev)
            )
        return copies

    def finish_reduce(q, ph, copies):
        a = plans[q][ph]
        g = size[a]
        m = span[q] // g
        for c in copies:
            c.wait()
        mine = rows_of(off[q] + at[a] * m, m) if ph == 0 else rows_of(at[a] * m, m)
        total = (w_ref[mine] if ph == 0 else held[q][ph - 1][mine]).astype(F32)
        for k in range(g - 1):
            total = total + stage[q][ph][k].astype(F32)
        off[q] = off[q] + at[a] * m
        span[q] = m
        if ph < len(plans[q]) - 1:
            held[q][ph][...] = total.astype(BF16)
        else:
            wout[core, rows_of(off[q], m)] = total.astype(BF16)

    def start_sums(ph):
        a = "xyz"[ph]
        width = stride[a]
        first = me // width * width
        block = pl.ds(first, width)
        return [
            remote(sout.at[block], sout.at[block], s_send.at[ph, k - 1], s_recv.at[ph, k - 1], peer(a, k)[1])
            for k in range(1, size[a])
        ]

    sout[me] = s_ref[...]
    bout[core] = b_ref[...]
    pending = [start_reduce(q, 0) for q in range(STREAMS)]
    sums = start_sums(0)
    basis_copy = remote(b_ref, bout.at[core], c_send.at[STREAMS], c_recv.at[STREAMS], partner)
    for ph in range(3):
        for c in sums:
            c.wait()
        if ph < 2:
            sums = start_sums(ph + 1)
        for q in range(STREAMS):
            finish_reduce(q, ph, pending[q])
            if ph < 2:
                pending[q] = start_reduce(q, ph + 1)

    def start_gather(q, ph):
        a = plans[q][ph]
        block = wout.at[core, rows_of(off[q], span[q])]
        return [
            remote(block, block, w_send.at[q, 3 + ph, k - 1], w_recv.at[q, 3 + ph, k - 1], peer(a, k)[1])
            for k in range(1, size[a])
        ]

    pending = [start_gather(q, 2) for q in range(STREAMS)]
    across = []
    for ph in (2, 1, 0):
        for q in range(STREAMS):
            a = plans[q][ph]
            for c in pending[q]:
                c.wait()
            off[q] = off[q] - at[a] * span[q]
            span[q] = span[q] * size[a]
            if ph > 0:
                pending[q] = start_gather(q, ph - 1)
            if ph == 1:
                early = rows_of(off[q], span[q])
                block = wout.at[core, early]
                across.append(remote(block, block, c_send.at[q], c_recv.at[q], partner))
            if ph == 0:
                part = span[q] // size[a]
                for k in range(1, size[a]):
                    p = peer(a, k)[0]
                    block = wout.at[core, rows_of(off[q] + p * part, part)]
                    sem = STREAMS + q * (size[a] - 1) + k
                    across.append(remote(block, block, c_send.at[sem], c_recv.at[sem], partner))
    for c in across:
        c.wait()
    basis_copy.wait()


def reduce(r, w, s, b):
    length = w.shape[0]
    nz, ny, nx = factors(r)
    stages, helds = [], []
    for sizes in ((nx, ny, nz), (ny, nx, nz)) * (STREAMS // 2):
        m = length // STREAMS
        for ph, g in enumerate(sizes):
            m //= g
            stages.append(pltpu.VMEM((max(g - 1, 1), m, LANES), BF16))
            if ph < 2:
                helds.append(pltpu.VMEM((m, LANES), BF16))
    widest = max(nx, ny, nz) - 1
    sems = ((STREAMS, 6, widest), (3, widest), (1 + STREAMS * (1 + widest),))
    vm = pl.BlockSpec(memory_space=pltpu.VMEM)
    dma = pltpu.SemaphoreType.DMA
    return pl.pallas_call(
        functools.partial(reduce_kernel, r),
        in_specs=[vm] * 3,
        out_specs=[vm] * 3,
        out_shape=[
            jax.ShapeDtypeStruct((2,) + w.shape, BF16),
            jax.ShapeDtypeStruct((r,) + s.shape, F32),
            jax.ShapeDtypeStruct((2,) + b.shape, BF16),
        ],
        scratch_shapes=stages + helds + [dma(shape) for shape in sems for _ in range(2)],
        compiler_params=pltpu.CompilerParams(collective_id=0, has_side_effects=True),
    )(w, s, b)


def shards(embeddings, start_basis):
    n, d = embeddings.shape
    total = n * lax.axis_size("rows")
    w, s = scatter(embeddings)
    shape = w.shape
    w, s, b = reduce(lax.axis_size("rows"), w.reshape(-1, LANES), s, start_basis.astype(BF16))
    w = w.reshape((2,) + shape)
    basis = iterate(n, total, w, s, b)
    return project(total, embeddings, s, basis, start_basis.shape[1])


def solution(mesh):
    in_specs = (P("rows", None), P(None, "cols"))
    out_specs = (P("rows", "cols"), P(None, "cols"))
    return jax.shard_map(shards, mesh=mesh, in_specs=in_specs, out_specs=out_specs, check_vma=False)
```

```python
import functools

import jax
import jax.numpy as jnp
from jax import lax
from jax.experimental import pallas as pl
from jax.experimental.pallas import tpu as pltpu
from jax.sharding import PartitionSpec as P

ITERS = 3
PARTS = 3
LANES = 128
MESH = pl.DeviceIdType.MESH
STREAMS = 2 * PARTS
TILES = 4
HI = lax.Precision.HIGHEST
F32 = jnp.float32
BF16 = jnp.bfloat16


def dot(a, b, ca, cb, precision=None):
    return lax.dot_general(a, b, (((ca,), (cb,)), ((), ())), precision=precision, preferred_element_type=F32)


BLOCKS = (((0, 0), (0, 1), (0, 2)), ((1, 1), (1, 2), (2, 2)))


def split(v):
    hi = v.astype(BF16)
    return hi, (v - hi.astype(F32)).astype(BF16)


def pivot_inverse(a):
    m = len(a)
    a = [list(row) for row in a]
    t = [[None] * m for _ in range(m)]
    inv = []
    for j in range(m):
        r = 1.0 / a[j][j]
        inv.append(r)
        for i in range(j + 1, m):
            f = a[i][j] * r
            for c in range(j + 1, i + 1):
                a[i][c] = a[i][c] - f * a[c][j]
            for c in range(j):
                t[i][c] = t[i][c] - f * t[j][c]
            t[i][j] = -f
    return t, inv


def inverse_factor(a_ref, k, b):
    w = 2 * b
    sub = lax.broadcasted_iota(jnp.int32, (8, w), 0)
    eye = (lax.broadcasted_iota(jnp.int32, (b, b), 0) == lax.broadcasted_iota(jnp.int32, (b, b), 1)).astype(F32)
    for blk in range(k // b):
        lo, hi = blk * b, (blk + 1) * b
        aug = jnp.concatenate([a_ref[lo:hi, lo:hi], eye], axis=1)
        tiles = [aug[8 * t:8 * t + 8] for t in range(b // 8)]
        for p in range(b // 8):
            cols = {
                t: [jnp.broadcast_to(tiles[t][:, 8 * p + c:8 * p + c + 1], (8, w)) for c in range(8)]
                for t in range(p, b // 8)
            }
            block = [[jnp.broadcast_to(cols[p][j][i:i + 1], (8, w)) for j in range(i + 1)] for i in range(8)]
            t8, inv = pivot_inverse(block)
            rows = [jnp.broadcast_to(tiles[p][c:c + 1], (8, w)) for c in range(8)]
            low = []
            for i in range(8):
                v = rows[i]
                for c in range(i):
                    v = v + t8[i][c] * rows[c]
                low.append(v)
            scaled = [low[i] * inv[i] for i in range(8)]
            if p + 1 < b // 8:
                solved = []
                for c in range(8):
                    v = scaled[c]
                    for i in range(c + 1, 8):
                        v = v + t8[i][c] * scaled[i]
                    solved.append(v)
                for t in range(p + 1, b // 8):
                    u = [cols[t][c] * solved[c] for c in range(8)]
                    tiles[t] = tiles[t] - (((u[0] + u[1]) + (u[2] + u[3])) + ((u[4] + u[5]) + (u[6] + u[7])))
            v, d = low[0], inv[0]
            for i in range(1, 8):
                v = jnp.where(sub == i, low[i], v)
                d = jnp.where(sub == i, inv[i], d)
            root = lax.rsqrt(d)
            root = root * (1.5 - 0.5 * d * root * root)
            tiles[p] = v * (d * root)
        strip = dot(jnp.concatenate(tiles, axis=0)[:, b:], a_ref[lo:hi, :], 1, 0, HI)
        a_ref[lo:hi, :] = strip
        if hi < k:
            a_ref[hi:, :] -= dot(strip[:, hi:k], strip, 0, 0, HI)


def iterate_kernel(n, total, w_ref, s_ref, b_ref, out_ref, w, basis, mean, mean_t, a):
    d, k = out_ref.shape
    t = d // PARTS
    for c, pairs in enumerate(BLOCKS):
        for slot, (i, j) in enumerate(pairs):
            v = jnp.concatenate([w_ref[c, slot, l] for l in range(t // LANES)], axis=1)
            w[i * t:(i + 1) * t, j * t:(j + 1) * t] = v
            if i != j:
                w[j * t:(j + 1) * t, i * t:(i + 1) * t] = v.T
    s = s_ref[:, 0, :]
    r = s.shape[0]
    m = s * (1.0 / n) - jnp.sum(s, axis=0, keepdims=True) * (1.0 / total)
    mh, ml = split(m)
    mean[:r] = mh
    mean[r:] = ml
    mean_t[...] = jnp.concatenate([mh.astype(F32), ml.astype(F32), mh.astype(F32)], axis=0).T.astype(BF16)
    basis[...] = jnp.concatenate([b_ref[0], b_ref[1]], axis=1)

    @pl.loop(0, ITERS)
    def _(_):
        bf = basis[...]
        inner = dot(mean[...], bf, 1, 0)
        ih, il = split((inner[:r] + inner[r:]) * float(n))
        ph, plo = split(dot(w[...], bf, 1, 0) + dot(mean_t[...], jnp.concatenate([ih, ih, il], axis=0), 1, 0))
        cross = dot(plo, ph, 0, 0)
        a[:, :k] = dot(ph, ph, 0, 0) + (dot(plo, plo, 0, 0) + (cross + cross.T))
        a[:, k:] = (
            lax.broadcasted_iota(jnp.int32, (k, k), 0) == lax.broadcasted_iota(jnp.int32, (k, k), 1)
        ).astype(F32)
        inverse_factor(a, k, 64)
        lh, ll = split(a[:, k:])
        new = dot(ph, lh, 1, 1) + (dot(ph, ll, 1, 1) + dot(plo, lh, 1, 1))
        out_ref[...] = new
        basis[...] = new.astype(BF16)


def iterate(n, total, w, s, b):
    d, k = b.shape[1], 2 * b.shape[2]
    vm = pl.BlockSpec(memory_space=pltpu.VMEM)
    return pl.pallas_call(
        functools.partial(iterate_kernel, n, total),
        in_specs=[vm] * 3,
        out_specs=vm,
        out_shape=jax.ShapeDtypeStruct((d, k), F32),
        scratch_shapes=[
            pltpu.VMEM((d, d), BF16),
            pltpu.VMEM((d, k), BF16),
            pltpu.VMEM((2 * s.shape[0], d), BF16),
            pltpu.VMEM((d, 3 * s.shape[0]), BF16),
            pltpu.VMEM((k, 2 * k), F32),
        ],
    )(w, s, b)


def project_kernel(total, e_ref, s_ref, b_ref, o_ref, basis_ref, mean, bf):
    core = lax.axis_index("cols")
    h = o_ref.shape[1]

    @pl.when(pl.program_id(0) == 0)
    def _():
        mean[...] = jnp.sum(s_ref[:, 0, :], axis=0, keepdims=True) * (1.0 / total)
        full = b_ref[...]
        bf[...] = full.astype(BF16)
        basis_ref[...] = jnp.where(core == 0, full[:, :h], full[:, h:])

    centered = e_ref[...].astype(F32) - mean[...]
    unit = (centered * lax.rsqrt(jnp.sum(centered * centered, axis=1, keepdims=True) + 1.0)).astype(BF16)
    coords = dot(unit, bf[...], 1, 0)
    k = coords.shape[1]
    scale = lax.rsqrt(jnp.sum(coords * coords, axis=1, keepdims=True) * (1.0 / k) + 0.0001)
    o_ref[...] = (jnp.where(core == 0, coords[:, :h], coords[:, h:]) * scale).astype(o_ref.dtype)


def project(total, e, s, b, h, rows=512):
    n, d = e.shape
    k = b.shape[1]
    return pl.pallas_call(
        functools.partial(project_kernel, total),
        grid=(n // rows,),
        in_specs=[
            pl.BlockSpec((rows, d), lambda i: (i, 0)),
            pl.BlockSpec(s.shape, lambda i: (0, 0, 0)),
            pl.BlockSpec((d, k), lambda i: (0, 0)),
        ],
        out_specs=[pl.BlockSpec((rows, h), lambda i: (i, 0)), pl.BlockSpec((d, h), lambda i: (0, 0))],
        out_shape=[jax.ShapeDtypeStruct((n, h), BF16), jax.ShapeDtypeStruct((d, h), F32)],
        scratch_shapes=[pltpu.VMEM((1, d), F32), pltpu.VMEM((d, k), BF16)],
    )(e, s, b)


def factors(r):
    z = 4 if r % 4 == 0 else 1
    x = 1
    while x * x < r // z:
        x *= 2
    return z, r // z // x, x


def reduce_kernel(r, e_hbm, b_ref, wout, sout, bout, e, acc, ssum, w_ref, e_sem, *scratch):
    nz, ny, nx = factors(r)
    plans = (("x", "y", "z"), ("y", "x", "z")) * (STREAMS // 2)
    size = {"x": nx, "y": ny, "z": nz}
    stride = {"x": 1, "y": nx, "z": nx * ny}
    scratch = list(scratch)
    stage = [[scratch.pop(0) for _ in plan] for plan in plans]
    held = [[scratch.pop(0) for _ in plan[:-1]] for plan in plans]
    w_send, w_recv, s_send, s_recv, c_send, c_recv = scratch

    me = lax.axis_index("rows")
    core = lax.axis_index("cols")
    n, d = e.shape
    t = d // PARTS
    tile = n // TILES

    def tile_copy(i):
        at_rows = pl.ds(pl.multiple_of(i * tile, tile), tile)
        return pltpu.make_async_copy(e_hbm.at[at_rows], e.at[at_rows], e_sem.at[i])

    for i in range(TILES):
        tile_copy(i).start()
    at = {a: lax.rem(me // stride[a], size[a]) for a in size}
    partner = {"cols": 1 - core}

    def peer(a, k):
        p = lax.rem(at[a] + k, size[a])
        return p, {"rows": me + (p - at[a]) * stride[a]}

    barrier = pltpu.get_barrier_semaphore()
    count = 1
    pl.semaphore_signal(barrier, inc=1, device_id=partner, device_id_type=MESH)
    for a in size:
        for k in range(1, size[a]):
            pl.semaphore_signal(barrier, inc=1, device_id=peer(a, k)[1], device_id_type=MESH)
            count += 1
    pl.semaphore_wait(barrier, count)

    def remote(src, dst, send, recv, device):
        copy = pltpu.make_async_remote_copy(
            src_ref=src, dst_ref=dst, send_sem=send, recv_sem=recv, device_id=device, device_id_type=MESH
        )
        copy.start()
        return copy

    def rows_of(off, m):
        return pl.ds(pl.multiple_of(off, 16), m)

    length = w_ref.shape[0]
    off = [q * (length // STREAMS) for q in range(STREAMS)]
    span = [length // STREAMS] * STREAMS

    def start_reduce(q, ph):
        a = plans[q][ph]
        g = size[a]
        m = span[q] // g
        copies = []
        for k in range(1, g):
            p, dev = peer(a, k)
            src = w_ref.at[rows_of(off[q] + p * m, m)] if ph == 0 else held[q][ph - 1].at[rows_of(p * m, m)]
            copies.append(
                remote(src, stage[q][ph].at[k - 1], w_send.at[q, ph, k - 1], w_recv.at[q, ph, k - 1], dev)
            )
        return copies

    def finish_reduce(q, ph, copies):
        a = plans[q][ph]
        g = size[a]
        m = span[q] // g
        for c in copies:
            c.wait()
        mine = rows_of(off[q] + at[a] * m, m) if ph == 0 else rows_of(at[a] * m, m)
        total = (w_ref[mine] if ph == 0 else held[q][ph - 1][mine]).astype(F32)
        for k in range(g - 1):
            total = total + stage[q][ph][k].astype(F32)
        off[q] = off[q] + at[a] * m
        span[q] = m
        if ph < len(plans[q]) - 1:
            held[q][ph][...] = total.astype(BF16)
        else:
            wout[core, rows_of(off[q], m)] = total.astype(BF16)

    def start_sums(ph):
        a = "xyz"[ph]
        width = stride[a]
        first = me // width * width
        block = pl.ds(first, width)
        return [
            remote(sout.at[block], sout.at[block], s_send.at[ph, k - 1], s_recv.at[ph, k - 1], peer(a, k)[1])
            for k in range(1, size[a])
        ]

    bout[core] = b_ref[...]
    basis_copy = remote(b_ref, bout.at[core], c_send.at[STREAMS], c_recv.at[STREAMS], partner)
    ssum[...] = jnp.zeros_like(ssum)
    pending = []
    for slot in range(PARTS):
        acc[...] = jnp.zeros_like(acc)
        for c in range(2):
            @pl.when(core == c)
            def _(slot=slot, c=c):
                i, j = BLOCKS[c][slot]

                @pl.loop(0, TILES)
                def _(step):
                    if slot == 0:
                        tile_copy(step).wait()
                    part = pl.ds(pl.multiple_of(step * tile, tile), tile)
                    if slot == 0:
                        ssum[...] += dot(jnp.ones((8, tile), BF16), e[part, :], 1, 0)
                    acc[...] += dot(e[part, i * t:(i + 1) * t], e[part, j * t:(j + 1) * t], 0, 0)

                si = ssum[:, i * t:(i + 1) * t] * (1.0 / (8 * n))
                v = (acc[...] - dot(si, ssum[:, j * t:(j + 1) * t], 0, 0, HI)).astype(BF16)
                for l in range(t // LANES):
                    first = (slot * (t // LANES) + l) * t
                    w_ref[first:first + t, :] = v[:, l * LANES:(l + 1) * LANES]

        if slot == 0:
            sout[me] = ssum[0:1, :]
        pending += [start_reduce(q, 0) for q in (2 * slot, 2 * slot + 1)]
        if slot == 0:
            sums = start_sums(0)
        else:
            for q in (2 * slot - 2, 2 * slot - 1):
                finish_reduce(q, 0, pending[q])
                pending[q] = start_reduce(q, 1)
    for ph in range(3):
        for c in sums:
            c.wait()
        if ph < 2:
            sums = start_sums(ph + 1)
        for q in range(STREAMS):
            if ph == 0 and q < STREAMS - 2:
                continue
            finish_reduce(q, ph, pending[q])
            if ph < 2:
                pending[q] = start_reduce(q, ph + 1)

    def start_gather(q, ph):
        a = plans[q][ph]
        block = wout.at[core, rows_of(off[q], span[q])]
        return [
            remote(block, block, w_send.at[q, 3 + ph, k - 1], w_recv.at[q, 3 + ph, k - 1], peer(a, k)[1])
            for k in range(1, size[a])
        ]

    pending = [start_gather(q, 2) for q in range(STREAMS)]
    across = []
    for ph in (2, 1, 0):
        for q in range(STREAMS):
            a = plans[q][ph]
            for c in pending[q]:
                c.wait()
            off[q] = off[q] - at[a] * span[q]
            span[q] = span[q] * size[a]
            if ph > 0:
                pending[q] = start_gather(q, ph - 1)
            if ph == 1:
                early = rows_of(off[q], span[q])
                block = wout.at[core, early]
                across.append(remote(block, block, c_send.at[q], c_recv.at[q], partner))
            if ph == 0:
                part = span[q] // size[a]
                for k in range(1, size[a]):
                    p = peer(a, k)[0]
                    block = wout.at[core, rows_of(off[q] + p * part, part)]
                    sem = STREAMS + q * (size[a] - 1) + k
                    across.append(remote(block, block, c_send.at[sem], c_recv.at[sem], partner))
    for c in across:
        c.wait()
    basis_copy.wait()


def reduce(r, e, b):
    n, d = e.shape
    t = d // PARTS
    length = PARTS * t * t // LANES
    nz, ny, nx = factors(r)
    stages, helds = [], []
    for sizes in ((nx, ny, nz), (ny, nx, nz)) * (STREAMS // 2):
        m = length // STREAMS
        for ph, g in enumerate(sizes):
            m //= g
            stages.append(pltpu.VMEM((max(g - 1, 1), m, LANES), BF16))
            if ph < 2:
                helds.append(pltpu.VMEM((m, LANES), BF16))
    widest = max(nx, ny, nz) - 1
    sems = ((STREAMS, 6, widest), (3, widest), (1 + STREAMS * (1 + widest),))
    vm = pl.BlockSpec(memory_space=pltpu.VMEM)
    dma = pltpu.SemaphoreType.DMA
    return pl.pallas_call(
        functools.partial(reduce_kernel, r),
        in_specs=[pl.BlockSpec(memory_space=pl.ANY), vm],
        out_specs=[vm] * 3,
        out_shape=[
            jax.ShapeDtypeStruct((2, length, LANES), BF16),
            jax.ShapeDtypeStruct((r, 1, d), F32),
            jax.ShapeDtypeStruct((2,) + b.shape, BF16),
        ],
        scratch_shapes=[
            pltpu.VMEM((n, d), BF16),
            pltpu.VMEM((t, t), F32),
            pltpu.VMEM((8, d), F32),
            pltpu.VMEM((length, LANES), BF16),
            dma((TILES,)),
        ]
        + stages + helds + [dma(shape) for shape in sems for _ in range(2)],
        compiler_params=pltpu.CompilerParams(collective_id=0, has_side_effects=True),
    )(e, b)


def shards(embeddings, start_basis):
    n, d = embeddings.shape
    total = n * lax.axis_size("rows")
    t = d // PARTS
    w, s, b = reduce(lax.axis_size("rows"), embeddings, start_basis.astype(BF16))
    w = w.reshape(2, PARTS, t // LANES, t, LANES)
    basis = iterate(n, total, w, s, b)
    return project(total, embeddings, s, basis, start_basis.shape[1])


def solution(mesh):
    in_specs = (P("rows", None), P(None, "cols"))
    out_specs = (P("rows", "cols"), P(None, "cols"))
    return jax.shard_map(shards, mesh=mesh, in_specs=in_specs, out_specs=out_specs, check_vma=False)
```
